32 devices in a mesh: expert: 4 (over x, core), shard: 8 (over z, y).
Axes of the slice: x: 2, y: 2, z: 4, core: 2. Of those that a mesh axis runs over, the one named last changes fastest.
Arguments:
- master_gate: float32 [128, 2048, 768], P('expert', 'shard'), may hold values from -0.125 to 0.125
- master_up: float32 [128, 2048, 768], P('expert', 'shard'), may hold values from -0.125 to 0.125
- router_weight: float32 [2048, 128], P('shard', 'expert'), may hold values from -0.125 to 0.125
- router_gain: float32 [2048], P('shard'), may hold values from 0.25 to 1.75
Outputs:
- final_gate: bfloat16 [128, 768, 2048], P('expert', 'shard')
- final_up: bfloat16 [128, 768, 2048], P('expert', 'shard')
- serve_router: bfloat16 [2048, 128], replicated
The draws below stay inside these ranges and needn't reach their ends.
All inputs are finite; a program needn't handle non-finite values.
Results may differ from the reference program's by a relative error of at most 0.001.
Values may be sent and summed in bfloat16 or wider, within the bound.
A program may use at most 192 MiB of HBM per device.

```python
import jax
import jax.numpy as jnp

EXPERTS = 128
D_MODEL = 2048
D_EXPERT = 768


def shard_levels(key, extent, shards, least, largest):
    gain, own = 1.0, jax.random.fold_in(key, 6)
    for axis_at, shards_of in shards:
        heights = jnp.exp(jax.random.uniform(jax.random.fold_in(own, axis_at), (shards_of,), jnp.float32, least / len(shards), largest / len(shards)))
        gain = gain * jnp.repeat(heights, extent[axis_at] // shards_of).reshape([-1 if axis == axis_at else 1 for axis in range(len(extent))])
    return gain


def centred(key, extent, width, most, split=(), dtype=jnp.bfloat16):
    array = width * jax.random.normal(key, extent, jnp.float32)
    if split:
        array = array * shard_levels(key, extent, split, -0.22, 0.18)
    return jnp.clip(array, -most, most).astype(dtype)


def setup_inputs(seed: int = 0) -> dict:
    key_list = jax.random.split(jax.random.key(seed), 5)
    master_gate = centred(key_list[0], (EXPERTS, D_MODEL, D_EXPERT), D_MODEL ** -0.5, 0.125, ((0, 4), (1, 8)), jnp.float32)
    master_up = centred(key_list[1], (EXPERTS, D_MODEL, D_EXPERT), D_MODEL ** -0.5, 0.125, ((0, 4), (1, 8)), jnp.float32)
    router_weight = centred(key_list[2], (D_MODEL, EXPERTS), D_MODEL ** -0.5, 0.125, ((0, 8), (1, 4)), jnp.float32)
    router_gain = jnp.clip(1.0 + 0.15 * jax.random.normal(key_list[3], (D_MODEL,), jnp.float32), 0.25, 1.75)
    return {"master_gate": master_gate, "master_up": master_up, "router_weight": router_weight, "router_gain": router_gain}


def reference(master_gate, master_up, router_weight, router_gain):
    final_gate = master_gate.astype(jnp.bfloat16)
    final_gate = jnp.transpose(final_gate, (0, 2, 1))
    final_up = master_up.astype(jnp.bfloat16)
    final_up = jnp.transpose(final_up, (0, 2, 1))
    serve_router = (router_weight * router_gain[:, None]).astype(jnp.bfloat16)
    return final_gate, final_up, serve_router
```

```python
import functools

import jax
import jax.numpy as jnp
from jax import lax
from jax.experimental import pallas as pl
from jax.experimental.pallas import tpu as pltpu
from jax.sharding import PartitionSpec as P

NEAR = 1
PAIR = 2
CORES = 2
CHUNK = 1
WINDOW = 2
EVERY = 3
SLOTS = 4
LIMIT = 32
TAILS = (8, 2)
TAIL = max(TAILS)
PIECES = 4


def plain(master_gate, master_up, router_weight, router_gain):
    narrow_gate, narrow_up = (master_gate.astype(jnp.bfloat16), master_up.astype(jnp.bfloat16))
    final_gate, final_up = (
        lax.all_to_all(narrow_gate, "shard", split_axis=2, concat_axis=1, tiled=True),
        lax.all_to_all(narrow_up, "shard", split_axis=2, concat_axis=1, tiled=True),
    )
    final_gate = jnp.transpose(final_gate, (0, 2, 1))
    final_up = jnp.transpose(final_up, (0, 2, 1))
    part_router = (router_weight * router_gain[:, None]).astype(jnp.bfloat16)
    row_router = lax.all_gather(part_router, "shard", axis=0, tiled=True)
    serve_router = lax.all_gather(row_router, "expert", axis=1, tiled=True)
    return (final_gate, final_up, serve_router)


def columns(of, depth):
    return pl.ds(pl.multiple_of(of * depth, depth), depth)


def per_core(group, act):
    for core, tail in enumerate(TAILS):
        @pl.when(lax.rem(group, CORES) == core)
        def _():
            act(tail)


def to_peers(shards, me, least, most, act):
    place, side = me // PAIR, lax.rem(me, PAIR)
    for away in range(least, most + 1):
        for turned in range(0 if away else 1, PAIR):
            other = lax.rem(side + turned, PAIR)
            if away == 0:
                act(place * PAIR + other)
                continue

            @pl.when(place + away < shards // PAIR)
            def _():
                act((place + away) * PAIR + other)

            @pl.when(place >= away)
            def _():
                act((place - away) * PAIR + other)


def kernel(
    shards, groups, gate, up, weight, gain, out_gate, out_up, out_router, rest,
    held, coming, router, load_sem, own_sem, send_sem, recv_sem,
    row_send, row_recv, side_send, side_recv, column_send, column_recv, ready,
):
    me, group = lax.axis_index("shard"), lax.axis_index("expert")
    _, _, experts, rows, depth = held.shape
    width = weight.shape[0]
    places = shards // PAIR
    last = places - 1
    place, side = me // PAIR, lax.rem(me, PAIR)
    chunks, early = experts // CHUNK, experts - TAIL
    sources, outs = (gate, up), (out_gate, out_up)
    mine = columns(me, depth)
    my_part = pl.ds(pl.multiple_of(group * width, width), width)
    peers = functools.partial(to_peers, shards, me)
    above, below = place + 1 < places, place >= 1
    tail = TAILS[0]
    for core in range(1, CORES):
        tail = jnp.where(lax.rem(group, CORES) == core, TAILS[core], tail)
    total = 2 * chunks - tail // CHUNK

    barrier = pltpu.get_barrier_semaphore()
    peers(0, NEAR, lambda peer: pl.semaphore_signal(barrier, inc=1, device_id={"shard": peer}))
    for step in range(1, groups):
        pl.semaphore_signal(barrier, inc=1, device_id={"expert": lax.rem(group + step, groups)})

    def enter():
        sides = jnp.where(above, 1, 0) + jnp.where(below, 1, 0)
        pl.semaphore_wait(barrier, PAIR + groups - 2 + PAIR * sides)

    def tell(way, away):
        pl.semaphore_signal(
            ready.at[way, away], inc=1, device_id={"shard": me + (PAIR if way else -PAIR)}
        )

    def far_ready(away):
        @pl.when(place + away < places)
        def _():
            pl.semaphore_wait(ready.at[0, away], 1)

            @pl.when(below)
            def _():
                tell(0, away + 1)

        @pl.when(place >= away)
        def _():
            pl.semaphore_wait(ready.at[1, away], 1)

            @pl.when(above)
            def _():
                tell(1, away + 1)

    def load(which, expert):
        slot = lax.rem(expert, SLOTS)
        return pltpu.make_async_copy(sources[which].at[expert], coming.at[slot], load_sem.at[slot])

    def own(which, first, count):
        span = pl.ds(first, count)
        return pltpu.make_async_copy(
            held.at[which, me, span], outs[which].at[span, :, mine], own_sem
        )

    def send(which, peer, chunk):
        span = pl.ds(chunk * CHUNK, CHUNK)
        return pltpu.make_async_remote_copy(
            src_ref=held.at[which, peer, span],
            dst_ref=outs[which].at[span, :, mine],
            send_sem=send_sem.at[which * chunks + chunk],
            recv_sem=recv_sem.at[which * chunks + chunk],
            device_id={"shard": peer},
        )

    def settle(at):
        part = held.at[0, pl.ds(0, shards - 1), pl.ds(0, CHUNK)]
        pltpu.make_async_remote_copy(
            src_ref=part,
            dst_ref=part,
            send_sem=send_sem.at[at],
            recv_sem=recv_sem.at[at],
            device_id={"shard": lax.rem(me + 1, shards)},
        ).wait()

    def row(of, way):
        at = side * places + of
        return pltpu.make_async_remote_copy(
            src_ref=router.at[at, my_part],
            dst_ref=router.at[at, my_part],
            send_sem=row_send.at[of, way],
            recv_sem=row_recv.at[of],
            device_id={"shard": me + (PAIR if way else -PAIR)},
        )

    def pass_rows(away, act):
        @pl.when(above & (place >= away))
        def _():
            act(row(place - away, 1))

        @pl.when(below & (place + away < places))
        def _():
            act(row(place + away, 0))

    def rows_in(away):
        @pl.when(place >= away)
        def _():
            row(place - away, 1).wait_recv()

        @pl.when(place + away < places)
        def _():
            row(place + away, 0).wait_recv()

    def across(turned, of):
        part = router.at[pl.ds(of * places, places), my_part]
        other = lax.rem(side + turned, PAIR)
        return pltpu.make_async_remote_copy(
            src_ref=part,
            dst_ref=part,
            send_sem=side_send.at[other],
            recv_sem=side_recv.at[of],
            device_id={"shard": place * PAIR + other},
        )

    def column(peer, of):
        part = pl.ds(pl.multiple_of(of * width, width), width)
        return pltpu.make_async_remote_copy(
            src_ref=router.at[:, part],
            dst_ref=router.at[:, part],
            send_sem=column_send.at[peer],
            recv_sem=column_recv.at[of],
            device_id={"expert": peer},
        )

    def turn(which, expert):
        load(which, expert).wait()
        block = coming[lax.rem(expert, SLOTS)].T.astype(jnp.bfloat16)
        for peer in range(shards):
            held[which, peer, expert] = block[peer * rows:(peer + 1) * rows]
        if which == 1:
            @pl.when(expert >= early)
            def _():
                for peer in range(shards):
                    rest[peer, expert - early] = held[which, peer, expert]

        @pl.when(expert + SLOTS < experts)
        def _():
            load(which, expert + SLOTS).start()

    def turns(which, chunk):
        @pl.loop(0, CHUNK)
        def _(step):
            turn(which, chunk * CHUNK + step)

    def go(which, chunk):
        at = which * chunks + chunk
        if which == 1:
            settle(at - WINDOW)
        else:
            pl.when(at >= WINDOW)(lambda: settle(at - WINDOW))
        peers(NEAR, last, lambda peer: send(which, peer, chunk).start())
        peers(0, 0, lambda peer: send(which, peer, chunk).start())
        own(which, chunk * CHUNK, CHUNK).start()

    def pass_on(away):
        rows_in(away)
        pass_rows(away, lambda copy: copy.start())

    def pass_across():
        rows_in(last)
        for turned in range(1, PAIR):
            across(turned, side).start()

    def pass_columns():
        for turned in range(1, PAIR):
            across(turned, lax.rem(side + turned, PAIR)).wait_recv()
        for step in range(1, groups):
            column(lax.rem(group + step, groups), group).start()

    def write_router():
        for step in range(1, groups):
            peer = lax.rem(group + step, groups)
            column(peer, peer).wait_recv()
        for shard in range(shards):
            at = shard % PAIR * places + shard // PAIR
            out_router[shard * depth:(shard + 1) * depth] = router[at].T
        for away in range(last):
            pass_rows(away, lambda copy: copy.wait_send())
        for turned in range(1, PAIR):
            across(turned, side).wait_send()
        for step in range(1, groups):
            column(lax.rem(group + step, groups), group).wait_send()

    steps = [functools.partial(pass_on, away) for away in range(1, last)]
    steps += [pass_across, pass_columns, write_router]

    for first in range(SLOTS):
        load(0, first).start()
    router[side * places + place, my_part] = (weight[...] * gain[...]).astype(jnp.bfloat16)
    turns(0, 0)
    enter()

    @pl.when(above & below)
    def _():
        tell(0, 2)
        tell(1, 2)
    turns(0, 1)
    for away in range(NEAR, last + 1):
        if away > NEAR:
            far_ready(away)
        peers(away, away, lambda peer: send(0, peer, 0).start())
    peers(0, 0, lambda peer: send(0, peer, 0).start())
    own(0, 0, CHUNK).start()
    pass_rows(0, lambda copy: copy.start())

    @pl.loop(1, chunks - 1)
    def _(chunk):
        turns(0, chunk + 1)
        go(0, chunk)
        for at, act in enumerate(steps):
            pl.when(chunk == (at + 1) * EVERY)(act)
    for first in range(SLOTS):
        load(1, first).start()
    turns(1, 0)
    go(0, chunks - 1)

    @pl.loop(0, chunks)
    def _(chunk):
        pl.when(chunk + 1 < chunks)(lambda: turns(1, chunk + 1))
        pl.when(chunks + chunk < total)(lambda: go(1, chunk))

    @pl.loop(total - WINDOW, total)
    def _(at):
        settle(at)

    def finish(tail):
        own(0, 0, experts).wait()
        own(1, 0, experts - tail).wait()
    per_core(group, finish)


def second(shards, rest, token, out, own_sem, send_sem, recv_sem):
    del token
    me, group = lax.axis_index("shard"), lax.axis_index("expert")
    depth = rest.shape[3]
    last = shards // PAIR - 1
    peers = functools.partial(to_peers, shards, me)
    barrier = pltpu.get_barrier_semaphore()
    peers(0, last, lambda peer: pl.semaphore_signal(barrier, inc=1, device_id={"shard": peer}))
    pl.semaphore_wait(barrier, shards - 1)

    def send(peer, at):
        return pltpu.make_async_remote_copy(
            src_ref=rest.at[peer, at],
            dst_ref=out.at[at, :, columns(me, depth)],
            send_sem=send_sem.at[at],
            recv_sem=recv_sem.at[at],
            device_id={"shard": peer},
        )

    def settle(at):
        part = rest.at[pl.ds(0, shards - 1), 0]
        pltpu.make_async_remote_copy(
            src_ref=part,
            dst_ref=part,
            send_sem=send_sem.at[at],
            recv_sem=recv_sem.at[at],
            device_id={"shard": lax.rem(me + 1, shards)},
        ).wait()

    def exchange(tail):
        span = pl.ds(TAIL - tail, tail)
        for at in range(TAIL - tail, TAIL):
            if at - WINDOW >= TAIL - tail:
                settle(at - WINDOW)
            peers(1, last, lambda peer: send(peer, at).start())
            peers(0, 0, lambda peer: send(peer, at).start())
        own = pltpu.make_async_copy(rest.at[me, span], out.at[span, :, columns(me, depth)], own_sem)
        own.start()
        own.wait()
        for at in range(max(TAIL - WINDOW, TAIL - tail), TAIL):
            settle(at)
    per_core(group, exchange)


def put_out(gate, up, router, out_gate, out_up, out_router, token, sem):
    experts, early = gate.shape[0], gate.shape[0] - TAIL
    token[...] = jnp.zeros_like(token)

    def copy(source, out, first, count, at):
        span = pl.ds(first, count)
        return pltpu.make_async_copy(source.at[span], out.at[span], sem.at[at])

    copies = [pltpu.make_async_copy(router, out_router, sem.at[0])]
    for source, out, count in ((gate, out_gate, experts), (up, out_up, early)):
        for piece in range(PIECES):
            first = count * piece // PIECES
            copies.append(copy(source, out, first, count * (piece + 1) // PIECES - first, len(copies)))
    for one in copies:
        one.start()

    def more(tail):
        if tail < TAIL:
            one = copy(up, out_up, early, TAIL - tail, len(copies))
            one.start()
            one.wait()
    per_core(lax.axis_index("expert"), more)
    for one in copies:
        one.wait()


def put_rest(rest, already, out, sem):
    del already

    def put(tail):
        first = out.shape[0] - tail
        copies = [
            pltpu.make_async_copy(rest.at[TAIL - tail + at], out.at[first + at], sem.at[at])
            for at in range(tail)
        ]
        for one in copies:
            one.start()
        for one in copies:
            one.wait()
    per_core(lax.axis_index("expert"), put)


def per_device(shards, groups, master_gate, master_up, router_weight, router_gain):
    experts, depth, inner = master_gate.shape
    width = router_weight.shape[1]
    rows = inner // shards
    places = shards // PAIR
    if (
        shards % PAIR or depth % 128 or rows % 16 or width % 16 or experts % CHUNK or experts < 3 * TAIL
        or (width * groups) % 128 or groups % CORES
        or places < 2 or experts // CHUNK < (places + 2) * EVERY
    ):
        return plain(master_gate, master_up, router_weight, router_gain)
    anywhere = pl.BlockSpec(memory_space=pl.ANY)
    inside = pl.BlockSpec(memory_space=pltpu.VMEM)
    final = (experts, rows, shards * depth)
    dma = pltpu.SemaphoreType.DMA
    gate, up, router, rest = pl.pallas_call(
        functools.partial(kernel, shards, groups),
        out_shape=(
            pltpu.VMEM(final, jnp.bfloat16),
            pltpu.VMEM((experts - min(TAILS), *final[1:]), jnp.bfloat16),
            pltpu.VMEM((shards * depth, groups * width), jnp.bfloat16),
            pltpu.VMEM((shards, TAIL, rows, depth), jnp.bfloat16),
        ),
        in_specs=[anywhere, anywhere, inside, inside],
        out_specs=(inside,) * 4,
        scratch_shapes=[
            pltpu.VMEM((2, shards, experts, rows, depth), jnp.bfloat16),
            pltpu.VMEM((SLOTS, depth, inner), jnp.float32),
            pltpu.VMEM((shards, groups * width, depth), jnp.bfloat16),
            dma((SLOTS,)), dma, dma((2 * experts // CHUNK,)), dma((2 * experts // CHUNK,)),
            dma((places, 2)), dma((places,)), dma((PAIR,)), dma((PAIR,)), dma((groups,)), dma((groups,)),
            pltpu.SemaphoreType.REGULAR((2, places + 1)),
        ],
        compiler_params=pltpu.CompilerParams(
            collective_id=0, has_side_effects=True, vmem_limit_bytes=LIMIT * 2**20
        ),
    )(master_gate, master_up, router_weight.T, router_gain[None])
    out = jax.ShapeDtypeStruct(final, jnp.bfloat16)
    final_gate, most_up, serve_router, token = pl.pallas_call(
        put_out,
        out_shape=(
            out, out, jax.ShapeDtypeStruct(router.shape, router.dtype), pltpu.VMEM((8, 128), jnp.float32)
        ),
        in_specs=[inside] * 3,
        out_specs=(anywhere,) * 3 + (inside,),
        scratch_shapes=[dma((2 * PIECES + 2,))],
        compiler_params=pltpu.CompilerParams(vmem_limit_bytes=2**20),
    )(gate, up, router)
    last_up = pl.pallas_call(
        functools.partial(second, shards),
        out_shape=pltpu.VMEM((TAIL, *final[1:]), jnp.bfloat16),
        in_specs=[inside] * 2,
        out_specs=inside,
        scratch_shapes=[dma, dma((TAIL,)), dma((TAIL,))],
        compiler_params=pltpu.CompilerParams(
            collective_id=1, has_side_effects=True, vmem_limit_bytes=2**20
        ),
    )(rest, token)
    final_up = pl.pallas_call(
        put_rest,
        out_shape=out,
        in_specs=[inside, anywhere],
        out_specs=anywhere,
        input_output_aliases={1: 0},
        scratch_shapes=[dma((TAIL,))],
        compiler_params=pltpu.CompilerParams(vmem_limit_bytes=2**20),
    )(last_up, most_up)
    return final_gate, final_up, serve_router


def solution(mesh):
    placed = (
        P("expert", "shard", None),
        P("expert", "shard", None),
        P("shard", "expert"),
        P("shard"),
    )
    return jax.shard_map(
        functools.partial(per_device, mesh.shape["shard"], mesh.shape["expert"]),
        mesh=mesh,
        in_specs=placed,
        out_specs=(P("expert", "shard", None), P("expert", "shard", None), P()),
        check_vma=False,
    )
```

```python
import functools

import jax
import jax.numpy as jnp
from jax import lax
from jax.experimental import pallas as pl
from jax.experimental.pallas import tpu as pltpu
from jax.sharding import PartitionSpec as P

NEAR = 1
PAIR = 2
CORES = 2
WINDOW = 2
LATER = 4
LEAD = 6
EVERY = 3
SLOTS = 4
LIMIT = 32
TAILS = (7, 2)
TAIL = max(TAILS)
PIECES = 4


def plain(master_gate, master_up, router_weight, router_gain):
    narrow_gate, narrow_up = (master_gate.astype(jnp.bfloat16), master_up.astype(jnp.bfloat16))
    final_gate, final_up = (
        lax.all_to_all(narrow_gate, "shard", split_axis=2, concat_axis=1, tiled=True),
        lax.all_to_all(narrow_up, "shard", split_axis=2, concat_axis=1, tiled=True),
    )
    final_gate = jnp.transpose(final_gate, (0, 2, 1))
    final_up = jnp.transpose(final_up, (0, 2, 1))
    part_router = (router_weight * router_gain[:, None]).astype(jnp.bfloat16)
    row_router = lax.all_gather(part_router, "shard", axis=0, tiled=True)
    serve_router = lax.all_gather(row_router, "expert", axis=1, tiled=True)
    return (final_gate, final_up, serve_router)


def columns(of, depth):
    return pl.ds(pl.multiple_of(of * depth, depth), depth)


def per_core(group, act):
    for core, tail in enumerate(TAILS):
        @pl.when(lax.rem(group, CORES) == core)
        def _():
            act(tail)


def to_peers(shards, me, least, most, act):
    place, side = me // PAIR, lax.rem(me, PAIR)
    for away in range(least, most + 1):
        for turned in range(0 if away else 1, PAIR):
            other = lax.rem(side + turned, PAIR)
            if away == 0:
                act(place * PAIR + other)
                continue

            @pl.when(place + away < shards // PAIR)
            def _():
                act((place + away) * PAIR + other)

            @pl.when(place >= away)
            def _():
                act((place - away) * PAIR + other)


def kernel(
    shards, groups, gate, up, weight, gain, out, out_router, rest,
    held, coming, router, load_sem, own_sem, send_sem, recv_sem,
    row_send, row_recv, side_send, side_recv, column_send, column_recv, ready,
):
    me, group = lax.axis_index("shard"), lax.axis_index("expert")
    _, units, rows, depth = held.shape
    experts = units // 2
    width = weight.shape[0]
    places = shards // PAIR
    last = places - 1
    place, side = me // PAIR, lax.rem(me, PAIR)
    early = units - TAIL
    mine = columns(me, depth)
    my_part = pl.ds(pl.multiple_of(group * width, width), width)
    peers = functools.partial(to_peers, shards, me)
    above, below = place + 1 < places, place >= 1
    tail = TAILS[0]
    for core in range(1, CORES):
        tail = jnp.where(lax.rem(group, CORES) == core, TAILS[core], tail)
    total = units - tail

    barrier = pltpu.get_barrier_semaphore()
    peers(0, NEAR, lambda peer: pl.semaphore_signal(barrier, inc=1, device_id={"shard": peer}))
    for step in range(1, groups):
        pl.semaphore_signal(barrier, inc=1, device_id={"expert": lax.rem(group + step, groups)})

    def enter():
        sides = jnp.where(above, 1, 0) + jnp.where(below, 1, 0)
        pl.semaphore_wait(barrier, PAIR + groups - 2 + PAIR * sides)

    def tell(way, away):
        pl.semaphore_signal(
            ready.at[way, away], inc=1, device_id={"shard": me + (PAIR if way else -PAIR)}
        )

    def far_ready(away):
        @pl.when(place + away < places)
        def _():
            pl.semaphore_wait(ready.at[0, away], 1)

            @pl.when(below)
            def _():
                tell(0, away + 1)

        @pl.when(place >= away)
        def _():
            pl.semaphore_wait(ready.at[1, away], 1)

            @pl.when(above)
            def _():
                tell(1, away + 1)

    def load(at, act):
        slot = lax.rem(at, SLOTS)
        for which, source in enumerate((gate, up)):
            @pl.when(at < experts if which == 0 else (at >= experts) & (at < units))
            def _():
                act(pltpu.make_async_copy(
                    source.at[at - which * experts], coming.at[slot], load_sem.at[slot]
                ))

    def own(first, count):
        span = pl.ds(first, count)
        return pltpu.make_async_copy(held.at[me, span], out.at[span, :, mine], own_sem)

    def send(peer, at):
        return pltpu.make_async_remote_copy(
            src_ref=held.at[peer, at],
            dst_ref=out.at[at, :, mine],
            send_sem=send_sem.at[at],
            recv_sem=recv_sem.at[at],
            device_id={"shard": peer},
        )

    def settle(at):
        part = held.at[0, pl.ds(0, shards - 1)]
        pltpu.make_async_remote_copy(
            src_ref=part,
            dst_ref=part,
            send_sem=send_sem.at[at],
            recv_sem=recv_sem.at[at],
            device_id={"shard": lax.rem(me + 1, shards)},
        ).wait()

    def row(of, way):
        at = side * places + of
        return pltpu.make_async_remote_copy(
            src_ref=router.at[at, my_part],
            dst_ref=router.at[at, my_part],
            send_sem=row_send.at[of, way],
            recv_sem=row_recv.at[of],
            device_id={"shard": me + (PAIR if way else -PAIR)},
        )

    def pass_rows(away, act):
        @pl.when(above & (place >= away))
        def _():
            act(row(place - away, 1))

        @pl.when(below & (place + away < places))
        def _():
            act(row(place + away, 0))

    def rows_in(away):
        @pl.when(place >= away)
        def _():
            row(place - away, 1).wait_recv()

        @pl.when(place + away < places)
        def _():
            row(place + away, 0).wait_recv()

    def across(turned, of):
        part = router.at[pl.ds(of * places, places), my_part]
        other = lax.rem(side + turned, PAIR)
        return pltpu.make_async_remote_copy(
            src_ref=part,
            dst_ref=part,
            send_sem=side_send.at[other],
            recv_sem=side_recv.at[of],
            device_id={"shard": place * PAIR + other},
        )

    def column(peer, of):
        part = pl.ds(pl.multiple_of(of * width, width), width)
        return pltpu.make_async_remote_copy(
            src_ref=router.at[:, part],
            dst_ref=router.at[:, part],
            send_sem=column_send.at[peer],
            recv_sem=column_recv.at[of],
            device_id={"expert": peer},
        )

    def turn(at, more=(SLOTS,)):
        load(at, lambda copy: copy.wait())
        for ahead in more[:-1]:
            load(at + ahead, lambda copy: copy.start())
        block = coming[lax.rem(at, SLOTS)].T.astype(jnp.bfloat16)
        for peer in range(shards):
            held[peer, at] = block[peer * rows:(peer + 1) * rows]

        @pl.when(at >= early)
        def _():
            for peer in range(shards):
                rest[peer, at - early] = held[peer, at]
        load(at + more[-1], lambda copy: copy.start())

    def near(at):
        peers(NEAR, NEAR, lambda peer: send(peer, at).start())
        peers(0, 0, lambda peer: send(peer, at).start())
        own(at, 1).start()

    def far(at):
        peers(NEAR + 1, last, lambda peer: send(peer, at).start())

    def pass_on(away):
        rows_in(away)
        pass_rows(away, lambda copy: copy.start())

    def pass_across():
        rows_in(last)
        for turned in range(1, PAIR):
            across(turned, side).start()

    def pass_columns():
        for turned in range(1, PAIR):
            across(turned, lax.rem(side + turned, PAIR)).wait_recv()
        for step in range(1, groups):
            column(lax.rem(group + step, groups), group).start()

    def write_router():
        for step in range(1, groups):
            peer = lax.rem(group + step, groups)
            column(peer, peer).wait_recv()
        for shard in range(shards):
            at = shard % PAIR * places + shard // PAIR
            out_router[shard * depth:(shard + 1) * depth] = router[at].T
        for away in range(last):
            pass_rows(away, lambda copy: copy.wait_send())
        for turned in range(1, PAIR):
            across(turned, side).wait_send()
        for step in range(1, groups):
            column(lax.rem(group + step, groups), group).wait_send()

    steps = [functools.partial(pass_on, away) for away in range(1, last)]
    steps += [pass_across, pass_columns, write_router]

    load(0, lambda copy: copy.start())
    router[side * places + place, my_part] = (weight[...] * gain[...]).astype(jnp.bfloat16)
    turn(0, range(1, SLOTS + 1))
    enter()

    @pl.when(above & below)
    def _():
        tell(0, 2)
        tell(1, 2)
    near(0)
    pass_rows(0, lambda copy: copy.start())

    @pl.loop(1, LEAD + 1)
    def _(at):
        turn(at)
        pl.when(at < LEAD)(lambda: near(at))
    for away in range(NEAR + 1, last + 1):
        far_ready(away)

    @pl.loop(0, units)
    def _(at):
        pl.when(at + LEAD + 1 < units)(lambda: turn(at + LEAD + 1))

        @pl.when(at < total)
        def _():
            pl.when(at >= WINDOW)(lambda: settle(at - WINDOW))
            pl.when(at + LEAD < total)(lambda: near(at + LEAD))
            far(at)
        for step, act in enumerate(steps):
            pl.when(at == (step + 1) * EVERY)(act)

    @pl.loop(total - WINDOW, total)
    def _(at):
        settle(at)
    per_core(group, lambda tail: own(0, units - tail).wait())


def second(shards, rest, token, out, own_sem, send_sem, recv_sem):
    del token
    me, group = lax.axis_index("shard"), lax.axis_index("expert")
    depth = rest.shape[3]
    last = shards // PAIR - 1
    peers = functools.partial(to_peers, shards, me)
    barrier = pltpu.get_barrier_semaphore()
    peers(0, last, lambda peer: pl.semaphore_signal(barrier, inc=1, device_id={"shard": peer}))
    pl.semaphore_wait(barrier, shards - 1)

    def send(peer, at):
        return pltpu.make_async_remote_copy(
            src_ref=rest.at[peer, at],
            dst_ref=out.at[at, :, columns(me, depth)],
            send_sem=send_sem.at[at],
            recv_sem=recv_sem.at[at],
            device_id={"shard": peer},
        )

    def settle(at):
        part = rest.at[pl.ds(0, shards - 1), 0]
        pltpu.make_async_remote_copy(
            src_ref=part,
            dst_ref=part,
            send_sem=send_sem.at[at],
            recv_sem=recv_sem.at[at],
            device_id={"shard": lax.rem(me + 1, shards)},
        ).wait()

    def exchange(tail):
        span = pl.ds(TAIL - tail, tail)
        for at in range(TAIL - tail, TAIL):
            if at - LATER >= TAIL - tail:
                settle(at - LATER)
            peers(1, last, lambda peer: send(peer, at).start())
            peers(0, 0, lambda peer: send(peer, at).start())
        own = pltpu.make_async_copy(rest.at[me, span], out.at[span, :, columns(me, depth)], own_sem)
        own.start()
        own.wait()
        for at in range(max(TAIL - LATER, TAIL - tail), TAIL):
            settle(at)
    per_core(group, exchange)


def put_out(kept, router, out_gate, out_up, out_router, token, sem):
    experts = out_gate.shape[0]
    early = experts - TAIL
    token[...] = jnp.zeros_like(token)

    def copy(which, first, count, at):
        return pltpu.make_async_copy(
            kept.at[pl.ds(which * experts + first, count)],
            (out_gate, out_up)[which].at[pl.ds(first, count)],
            sem.at[at],
        )

    copies = [pltpu.make_async_copy(router, out_router, sem.at[0])]
    for which, count in enumerate((experts, early)):
        for piece in range(PIECES):
            first = count * piece // PIECES
            copies.append(copy(which, first, count * (piece + 1) // PIECES - first, len(copies)))
    for one in copies:
        one.start()

    def more(tail):
        if tail < TAIL:
            one = copy(1, early, TAIL - tail, len(copies))
            one.start()
            one.wait()
    per_core(lax.axis_index("expert"), more)
    for one in copies:
        one.wait()


def put_rest(rest, already, out, sem):
    del already

    def put(tail):
        first = out.shape[0] - tail
        copies = [
            pltpu.make_async_copy(rest.at[TAIL - tail + at], out.at[first + at], sem.at[at])
            for at in range(tail)
        ]
        for one in copies:
            one.start()
        for one in copies:
            one.wait()
    per_core(lax.axis_index("expert"), put)


def per_device(shards, groups, master_gate, master_up, router_weight, router_gain):
    experts, depth, inner = master_gate.shape
    width = router_weight.shape[1]
    rows = inner // shards
    places = shards // PAIR
    if (
        shards % PAIR or depth % 128 or rows % 16 or width % 16 or experts < 3 * TAIL
        or (width * groups) % 128 or groups % CORES
        or places < 2 or experts < (places + 2) * EVERY
    ):
        return plain(master_gate, master_up, router_weight, router_gain)
    anywhere = pl.BlockSpec(memory_space=pl.ANY)
    inside = pl.BlockSpec(memory_space=pltpu.VMEM)
    final = (experts, rows, shards * depth)
    dma = pltpu.SemaphoreType.DMA
    kept, router, rest = pl.pallas_call(
        functools.partial(kernel, shards, groups),
        out_shape=(
            pltpu.VMEM((2 * experts - min(TAILS), *final[1:]), jnp.bfloat16),
            pltpu.VMEM((shards * depth, groups * width), jnp.bfloat16),
            pltpu.VMEM((shards, TAIL, rows, depth), jnp.bfloat16),
        ),
        in_specs=[anywhere, anywhere, inside, inside],
        out_specs=(inside,) * 3,
        scratch_shapes=[
            pltpu.VMEM((shards, 2 * experts, rows, depth), jnp.bfloat16),
            pltpu.VMEM((SLOTS, depth, inner), jnp.float32),
            pltpu.VMEM((shards, groups * width, depth), jnp.bfloat16),
            dma((SLOTS,)), dma, dma((2 * experts,)), dma((2 * experts,)),
            dma((places, 2)), dma((places,)), dma((PAIR,)), dma((PAIR,)), dma((groups,)), dma((groups,)),
            pltpu.SemaphoreType.REGULAR((2, places + 1)),
        ],
        compiler_params=pltpu.CompilerParams(
            collective_id=0, has_side_effects=True, vmem_limit_bytes=LIMIT * 2**20
        ),
    )(master_gate, master_up, router_weight.T, router_gain[None])
    out = jax.ShapeDtypeStruct(final, jnp.bfloat16)
    final_gate, most_up, serve_router, token = pl.pallas_call(
        put_out,
        out_shape=(
            out, out, jax.ShapeDtypeStruct(router.shape, router.dtype), pltpu.VMEM((8, 128), jnp.float32)
        ),
        in_specs=[inside] * 2,
        out_specs=(anywhere,) * 3 + (inside,),
        scratch_shapes=[dma((2 * PIECES + 2,))],
        compiler_params=pltpu.CompilerParams(vmem_limit_bytes=2**20),
    )(kept, router)
    kept_rest = pl.pallas_call(
        functools.partial(second, shards),
        out_shape=pltpu.VMEM((TAIL, *final[1:]), jnp.bfloat16),
        in_specs=[inside] * 2,
        out_specs=inside,
        scratch_shapes=[dma, dma((TAIL,)), dma((TAIL,))],
        compiler_params=pltpu.CompilerParams(
            collective_id=1, has_side_effects=True, vmem_limit_bytes=2**20
        ),
    )(rest, token)
    final_up = pl.pallas_call(
        put_rest,
        out_shape=out,
        in_specs=[inside, anywhere],
        out_specs=anywhere,
        input_output_aliases={1: 0},
        scratch_shapes=[dma((TAIL,))],
        compiler_params=pltpu.CompilerParams(vmem_limit_bytes=2**20),
    )(kept_rest, most_up)
    return final_gate, final_up, serve_router


def solution(mesh):
    placed = (
        P("expert", "shard", None),
        P("expert", "shard", None),
        P("shard", "expert"),
        P("shard"),
    )
    return jax.shard_map(
        functools.partial(per_device, mesh.shape["shard"], mesh.shape["expert"]),
        mesh=mesh,
        in_specs=placed,
        out_specs=(P("expert", "shard", None), P("expert", "shard", None), P()),
        check_vma=False,
    )
```

```python
import functools

import jax
import jax.numpy as jnp
from jax import lax
from jax.experimental import pallas as pl
from jax.experimental.pallas import tpu as pltpu
from jax.sharding import PartitionSpec as P

NEAR = 1
PAIR = 2
CORES = 2
WINDOW = 2
LATER = 4
LEAD = 16
EVERY = 3
SLOTS = 4
LIMIT = 32
TAILS = (6, 2)
TAIL = max(TAILS)
PIECES = 4


def plain(master_gate, master_up, router_weight, router_gain):
    narrow_gate, narrow_up = (master_gate.astype(jnp.bfloat16), master_up.astype(jnp.bfloat16))
    final_gate, final_up = (
        lax.all_to_all(narrow_gate, "shard", split_axis=2, concat_axis=1, tiled=True),
        lax.all_to_all(narrow_up, "shard", split_axis=2, concat_axis=1, tiled=True),
    )
    final_gate = jnp.transpose(final_gate, (0, 2, 1))
    final_up = jnp.transpose(final_up, (0, 2, 1))
    part_router = (router_weight * router_gain[:, None]).astype(jnp.bfloat16)
    row_router = lax.all_gather(part_router, "shard", axis=0, tiled=True)
    serve_router = lax.all_gather(row_router, "expert", axis=1, tiled=True)
    return (final_gate, final_up, serve_router)


def columns(of, depth):
    return pl.ds(pl.multiple_of(of * depth, depth), depth)


def per_core(group, act):
    for core, tail in enumerate(TAILS):
        @pl.when(lax.rem(group, CORES) == core)
        def _():
            act(tail)


def to_peers(shards, me, least, most, act):
    place, side = me // PAIR, lax.rem(me, PAIR)
    for away in range(least, most + 1):
        for turned in range(0 if away else 1, PAIR):
            other = lax.rem(side + turned, PAIR)
            if away == 0:
                act(place * PAIR + other)
                continue

            @pl.when(place + away < shards // PAIR)
            def _():
                act((place + away) * PAIR + other)

            @pl.when(place >= away)
            def _():
                act((place - away) * PAIR + other)


def kernel(
    shards, groups, gate, up, weight, gain, out, out_router, rest,
    held, coming, router, load_sem, own_sem, send_sem, recv_sem,
    row_send, row_recv, side_send, side_recv, column_send, column_recv, ready,
):
    me, group = lax.axis_index("shard"), lax.axis_index("expert")
    _, units, rows, depth = held.shape
    experts = units // 2
    width = weight.shape[0]
    places = shards // PAIR
    last = places - 1
    place, side = me // PAIR, lax.rem(me, PAIR)
    early = units - TAIL
    mine = columns(me, depth)
    my_part = pl.ds(pl.multiple_of(group * width, width), width)
    peers = functools.partial(to_peers, shards, me)
    above, below = place + 1 < places, place >= 1
    tail = TAILS[0]
    for core in range(1, CORES):
        tail = jnp.where(lax.rem(group, CORES) == core, TAILS[core], tail)
    total = units - tail

    barrier = pltpu.get_barrier_semaphore()
    peers(0, NEAR, lambda peer: pl.semaphore_signal(barrier, inc=1, device_id={"shard": peer}))
    for step in range(1, groups):
        pl.semaphore_signal(barrier, inc=1, device_id={"expert": lax.rem(group + step, groups)})

    def enter():
        sides = jnp.where(above, 1, 0) + jnp.where(below, 1, 0)
        pl.semaphore_wait(barrier, PAIR + groups - 2 + PAIR * sides)

    def tell(way, away):
        pl.semaphore_signal(
            ready.at[way, away], inc=1, device_id={"shard": me + (PAIR if way else -PAIR)}
        )

    def far_ready(away):
        @pl.when(place + away < places)
        def _():
            pl.semaphore_wait(ready.at[0, away], 1)

            @pl.when(below)
            def _():
                tell(0, away + 1)

        @pl.when(place >= away)
        def _():
            pl.semaphore_wait(ready.at[1, away], 1)

            @pl.when(above)
            def _():
                tell(1, away + 1)

    def load(at, act):
        slot = lax.rem(at, SLOTS)
        for which, source in enumerate((gate, up)):
            @pl.when(at < experts if which == 0 else (at >= experts) & (at < units))
            def _():
                act(pltpu.make_async_copy(
                    source.at[at - which * experts], coming.at[slot], load_sem.at[slot]
                ))

    def own(first, count):
        span = pl.ds(first, count)
        return pltpu.make_async_copy(held.at[me, span], out.at[span, :, mine], own_sem)

    def send(peer, at):
        return pltpu.make_async_remote_copy(
            src_ref=held.at[peer, at],
            dst_ref=out.at[at, :, mine],
            send_sem=send_sem.at[at],
            recv_sem=recv_sem.at[at],
            device_id={"shard": peer},
        )

    def settle(at):
        part = held.at[0, pl.ds(0, shards - 1)]
        pltpu.make_async_remote_copy(
            src_ref=part,
            dst_ref=part,
            send_sem=send_sem.at[at],
            recv_sem=recv_sem.at[at],
            device_id={"shard": lax.rem(me + 1, shards)},
        ).wait()

    def row(of, way):
        at = side * places + of
        return pltpu.make_async_remote_copy(
            src_ref=router.at[at, my_part],
            dst_ref=router.at[at, my_part],
            send_sem=row_send.at[of, way],
            recv_sem=row_recv.at[of],
            device_id={"shard": me + (PAIR if way else -PAIR)},
        )

    def pass_rows(away, act):
        @pl.when(above & (place >= away))
        def _():
            act(row(place - away, 1))

        @pl.when(below & (place + away < places))
        def _():
            act(row(place + away, 0))

    def rows_in(away):
        @pl.when(place >= away)
        def _():
            row(place - away, 1).wait_recv()

        @pl.when(place + away < places)
        def _():
            row(place + away, 0).wait_recv()

    def across(turned, of):
        part = router.at[pl.ds(of * places, places), my_part]
        other = lax.rem(side + turned, PAIR)
        return pltpu.make_async_remote_copy(
            src_ref=part,
            dst_ref=part,
            send_sem=side_send.at[other],
            recv_sem=side_recv.at[of],
            device_id={"shard": place * PAIR + other},
        )

    def column(peer, of):
        part = pl.ds(pl.multiple_of(of * width, width), width)
        return pltpu.make_async_remote_copy(
            src_ref=router.at[:, part],
            dst_ref=router.at[:, part],
            send_sem=column_send.at[peer],
            recv_sem=column_recv.at[of],
            device_id={"expert": peer},
        )

    def turn(at, more=(SLOTS,)):
        load(at, lambda copy: copy.wait())
        for ahead in more[:-1]:
            load(at + ahead, lambda copy: copy.start())
        block = coming[lax.rem(at, SLOTS)].T.astype(jnp.bfloat16)
        for peer in range(shards):
            held[peer, at] = block[peer * rows:(peer + 1) * rows]

        @pl.when(at >= early)
        def _():
            for peer in range(shards):
                rest[peer, at - early] = held[peer, at]
        load(at + more[-1], lambda copy: copy.start())

    def near(at):
        peers(NEAR, NEAR, lambda peer: send(peer, at).start())
        peers(0, 0, lambda peer: send(peer, at).start())
        own(at, 1).start()

    def far(at):
        peers(NEAR + 1, last, lambda peer: send(peer, at).start())

    def pass_on(away):
        rows_in(away)
        pass_rows(away, lambda copy: copy.start())

    def pass_across():
        rows_in(last)
        for turned in range(1, PAIR):
            across(turned, side).start()

    def pass_columns():
        for turned in range(1, PAIR):
            across(turned, lax.rem(side + turned, PAIR)).wait_recv()
        for step in range(1, groups):
            column(lax.rem(group + step, groups), group).start()

    def write_router():
        for step in range(1, groups):
            peer = lax.rem(group + step, groups)
            column(peer, peer).wait_recv()
        for shard in range(shards):
            at = shard % PAIR * places + shard // PAIR
            out_router[shard * depth:(shard + 1) * depth] = router[at].T
        for away in range(last):
            pass_rows(away, lambda copy: copy.wait_send())
        for turned in range(1, PAIR):
            across(turned, side).wait_send()
        for step in range(1, groups):
            column(lax.rem(group + step, groups), group).wait_send()

    steps = [functools.partial(pass_on, away) for away in range(1, last)]
    steps += [pass_across, pass_columns, write_router]

    load(0, lambda copy: copy.start())
    router[side * places + place, my_part] = (weight[...] * gain[...]).astype(jnp.bfloat16)
    turn(0, range(1, SLOTS + 1))
    enter()

    @pl.when(above & below)
    def _():
        tell(0, 2)
        tell(1, 2)
    near(0)
    pass_rows(0, lambda copy: copy.start())

    @pl.loop(1, LEAD + 1)
    def _(at):
        turn(at)
        pl.when(at < LEAD)(lambda: near(at))
    for away in range(NEAR + 1, last + 1):
        far_ready(away)

    @pl.loop(0, units)
    def _(at):
        pl.when(at + LEAD + 1 < units)(lambda: turn(at + LEAD + 1))

        @pl.when(at < total)
        def _():
            pl.when(at >= WINDOW)(lambda: settle(at - WINDOW))
            pl.when(at + LEAD < total)(lambda: near(at + LEAD))
            far(at)
        for step, act in enumerate(steps):
            pl.when(at == (step + 1) * EVERY)(act)

    @pl.loop(total - WINDOW, total)
    def _(at):
        settle(at)
    per_core(group, lambda tail: own(0, units - tail).wait())


def second(shards, rest, token, out, own_sem, send_sem, recv_sem):
    del token
    me, group = lax.axis_index("shard"), lax.axis_index("expert")
    depth = rest.shape[3]
    last = shards // PAIR - 1
    peers = functools.partial(to_peers, shards, me)
    barrier = pltpu.get_barrier_semaphore()
    peers(0, last, lambda peer: pl.semaphore_signal(barrier, inc=1, device_id={"shard": peer}))
    pl.semaphore_wait(barrier, shards - 1)

    def send(peer, at):
        return pltpu.make_async_remote_copy(
            src_ref=rest.at[peer, at],
            dst_ref=out.at[at, :, columns(me, depth)],
            send_sem=send_sem.at[at],
            recv_sem=recv_sem.at[at],
            device_id={"shard": peer},
        )

    def settle(at):
        part = rest.at[pl.ds(0, shards - 1), 0]
        pltpu.make_async_remote_copy(
            src_ref=part,
            dst_ref=part,
            send_sem=send_sem.at[at],
            recv_sem=recv_sem.at[at],
            device_id={"shard": lax.rem(me + 1, shards)},
        ).wait()

    def exchange(tail):
        span = pl.ds(TAIL - tail, tail)
        for at in range(TAIL - tail, TAIL):
            if at - LATER >= TAIL - tail:
                settle(at - LATER)
            peers(1, last, lambda peer: send(peer, at).start())
            peers(0, 0, lambda peer: send(peer, at).start())
        own = pltpu.make_async_copy(rest.at[me, span], out.at[span, :, columns(me, depth)], own_sem)
        own.start()
        own.wait()
        for at in range(max(TAIL - LATER, TAIL - tail), TAIL):
            settle(at)
    per_core(group, exchange)


def put_out(kept, router, out_gate, out_up, out_router, token, sem):
    experts = out_gate.shape[0]
    early = experts - TAIL
    token[...] = jnp.zeros_like(token)

    def copy(which, first, count, at):
        return pltpu.make_async_copy(
            kept.at[pl.ds(which * experts + first, count)],
            (out_gate, out_up)[which].at[pl.ds(first, count)],
            sem.at[at],
        )

    copies = [pltpu.make_async_copy(router, out_router, sem.at[0])]
    for which, count in enumerate((experts, early)):
        for piece in range(PIECES):
            first = count * piece // PIECES
            copies.append(copy(which, first, count * (piece + 1) // PIECES - first, len(copies)))
    for one in copies:
        one.start()

    def more(tail):
        if tail < TAIL:
            one = copy(1, early, TAIL - tail, len(copies))
            one.start()
            one.wait()
    per_core(lax.axis_index("expert"), more)
    for one in copies:
        one.wait()


def put_rest(rest, already, out, sem):
    del already

    def put(tail):
        first = out.shape[0] - tail
        copies = [
            pltpu.make_async_copy(rest.at[TAIL - tail + at], out.at[first + at], sem.at[at])
            for at in range(tail)
        ]
        for one in copies:
            one.start()
        for one in copies:
            one.wait()
    per_core(lax.axis_index("expert"), put)


def per_device(shards, groups, master_gate, master_up, router_weight, router_gain):
    experts, depth, inner = master_gate.shape
    width = router_weight.shape[1]
    rows = inner // shards
    places = shards // PAIR
    if (
        shards % PAIR or depth % 128 or rows % 16 or width % 16 or experts < 3 * TAIL
        or (width * groups) % 128 or groups % CORES
        or places < 2 or experts < (places + 2) * EVERY
    ):
        return plain(master_gate, master_up, router_weight, router_gain)
    anywhere = pl.BlockSpec(memory_space=pl.ANY)
    inside = pl.BlockSpec(memory_space=pltpu.VMEM)
    final = (experts, rows, shards * depth)
    dma = pltpu.SemaphoreType.DMA
    kept, router, rest = pl.pallas_call(
        functools.partial(kernel, shards, groups),
        out_shape=(
            pltpu.VMEM((2 * experts - min(TAILS), *final[1:]), jnp.bfloat16),
            pltpu.VMEM((shards * depth, groups * width), jnp.bfloat16),
            pltpu.VMEM((shards, TAIL, rows, depth), jnp.bfloat16),
        ),
        in_specs=[anywhere, anywhere, inside, inside],
        out_specs=(inside,) * 3,
        scratch_shapes=[
            pltpu.VMEM((shards, 2 * experts, rows, depth), jnp.bfloat16),
            pltpu.VMEM((SLOTS, depth, inner), jnp.float32),
            pltpu.VMEM((shards, groups * width, depth), jnp.bfloat16),
            dma((SLOTS,)), dma, dma((2 * experts,)), dma((2 * experts,)),
            dma((places, 2)), dma((places,)), dma((PAIR,)), dma((PAIR,)), dma((groups,)), dma((groups,)),
            pltpu.SemaphoreType.REGULAR((2, places + 1)),
        ],
        compiler_params=pltpu.CompilerParams(
            collective_id=0, has_side_effects=True, vmem_limit_bytes=LIMIT * 2**20
        ),
    )(master_gate, master_up, router_weight.T, router_gain[None])
    out = jax.ShapeDtypeStruct(final, jnp.bfloat16)
    final_gate, most_up, serve_router, token = pl.pallas_call(
        put_out,
        out_shape=(
            out, out, jax.ShapeDtypeStruct(router.shape, router.dtype), pltpu.VMEM((8, 128), jnp.float32)
        ),
        in_specs=[inside] * 2,
        out_specs=(anywhere,) * 3 + (inside,),
        scratch_shapes=[dma((2 * PIECES + 2,))],
        compiler_params=pltpu.CompilerParams(vmem_limit_bytes=2**20),
    )(kept, router)
    kept_rest = pl.pallas_call(
        functools.partial(second, shards),
        out_shape=pltpu.VMEM((TAIL, *final[1:]), jnp.bfloat16),
        in_specs=[inside] * 2,
        out_specs=inside,
        scratch_shapes=[dma, dma((TAIL,)), dma((TAIL,))],
        compiler_params=pltpu.CompilerParams(
            collective_id=1, has_side_effects=True, vmem_limit_bytes=2**20
        ),
    )(rest, token)
    final_up = pl.pallas_call(
        put_rest,
        out_shape=out,
        in_specs=[inside, anywhere],
        out_specs=anywhere,
        input_output_aliases={1: 0},
        scratch_shapes=[dma((TAIL,))],
        compiler_params=pltpu.CompilerParams(vmem_limit_bytes=2**20),
    )(kept_rest, most_up)
    return final_gate, final_up, serve_router


def solution(mesh):
    placed = (
        P("expert", "shard", None),
        P("expert", "shard", None),
        P("shard", "expert"),
        P("shard"),
    )
    return jax.shard_map(
        functools.partial(per_device, mesh.shape["shard"], mesh.shape["expert"]),
        mesh=mesh,
        in_specs=placed,
        out_specs=(P("expert", "shard", None), P("expert", "shard", None), P()),
        check_vma=False,
    )
```
